32 devices in a mesh: sub: 8 (over z, y), inner: 4 (over x, core).
Axes of the slice: x: 2, y: 2, z: 4, core: 2. Of those that a mesh axis runs over, the one named last changes fastest.
Arguments:
- solution: float32 [32, 3, 32, 16, 128], P(None, None, 'sub', 'inner'), may hold values from -6 to 6
- residual: float32 [32, 3, 32, 16, 128], P(None, None, 'sub', 'inner'), may hold values from -6 to 6
- direction: float32 [32, 3, 32, 16, 128], P(None, None, 'sub', 'inner'), may hold values from -6 to 6
- mass: float32 [32, 16, 128], P('sub', 'inner'), may hold values from 0.2 to 5
- coarse_basis: float32 [32, 3, 32, 16, 128], P(None, None, 'sub', 'inner'), may hold values from -1 to 1
- line_inverse: float32 [8, 4, 128, 128], P('sub', 'inner'), may hold values from -1.5 to 1.5
- coarse_factor: float32 [1024, 1024], P(('sub', 'inner')), may hold values from -1 to 1
Outputs:
- new_solution: float32 [32, 3, 32, 16, 128], P(None, None, 'sub', 'inner')
- new_residual: float32 [32, 3, 32, 16, 128], P(None, None, 'sub', 'inner')
- new_direction: float32 [32, 3, 32, 16, 128], P(None, None, 'sub', 'inner')
The draws below stay inside these ranges and needn't reach their ends.
All inputs are finite; a program needn't handle non-finite values.
Results may differ from the reference program's by a relative error of at most 0.00017.
Values sent between devices are 32-bit elements; how exact they have to be, the bound alone decides.
A program may use at most 64 MiB of HBM per device.

```python
import math
import jax
import jax.numpy as jnp
from jax import lax

K = 32
NB = 32
CX = 4
CY = 4
CZ = 128
NX = 32
NY = 16
NZ = 128
NCOARSE = 1024
N_SUB = 8
N_INNER = 4


def paired_fields(key):
    first = jax.random.fold_in(key, 31)
    second = jax.random.fold_in(key, 32)
    shape = (K, 3, NX, NY, NZ)
    base = jnp.clip(jax.random.normal(first, shape, jnp.float32), -6.0, 6.0)
    noise = jnp.clip(jax.random.normal(second, shape, jnp.float32), -4.0, 4.0)
    moved = jnp.clip(base + 0.3 * noise, -6.0, 6.0)
    return (base, moved)


def draw_residual(key, part):
    return paired_fields(key)[0]


def draw_direction(key, part):
    return paired_fields(key)[1]


def draw_coarse_basis(key, part):
    return jax.random.uniform(key, (NB, 3, NX, NY, NZ), jnp.float32, -1.0, 1.0)


def draw_line_inverse(key, part):
    first = jax.random.fold_in(key, 11)
    second = jax.random.fold_in(key, 12)
    diagonal = jax.random.uniform(first, (N_SUB, N_INNER, CZ), jnp.float32, 0.5, 1.5)
    noise = jnp.clip(jax.random.normal(second, (N_SUB, N_INNER, CZ, CZ), jnp.float32), -4.0, 4.0)
    symmetric = (noise + jnp.swapaxes(noise, 2, 3)) * (0.35 / CZ ** 0.5)
    eye = jnp.eye(CZ, dtype=jnp.float32)
    return symmetric * (1.0 - eye) + diagonal[..., None] * eye


def draw_coarse_factor(key, part):
    first = jax.random.fold_in(key, 21)
    second = jax.random.fold_in(key, 22)
    factor = 0.7 * (3.0 * CX * CY * CZ * NB) ** (-0.25)
    diagonal = jax.random.uniform(first, (NCOARSE,), jnp.float32, 0.5, 1.5)
    noise = jnp.clip(jax.random.normal(second, (NCOARSE, NCOARSE), jnp.float32), -4.0, 4.0)
    eye = jnp.eye(NCOARSE, dtype=jnp.float32)
    matrix = noise * (0.5 / NCOARSE ** 0.5) * (1.0 - eye) + diagonal[:, None] * eye
    return matrix * factor


def levels(own_key, dims, cuts, smallest, high):
    gain = 1.0
    for dim, parts in cuts:
        heights = jax.random.uniform(jax.random.fold_in(jax.random.fold_in(own_key, 6), dim), (parts,), jnp.float32, smallest / len(cuts), high / len(cuts))
        gain = gain * jnp.repeat(jnp.exp(heights), dims[dim] // parts).reshape((-1,) + (1,) * (len(dims) - 1 - dim))
    return gain


def scatter_about(stream_key, shape, deviation, most, split=(), held_as=jnp.bfloat16):
    entries = jax.random.normal(stream_key, shape, jnp.float32) * deviation
    if len(split) > 0:
        entries = levels(stream_key, shape, split, -0.22, 0.18) * entries
    return jnp.clip(entries, min=-most, max=most).astype(held_as)


def setup_inputs(seed: int = 0) -> dict:
    key_of = jax.random.split(jax.random.key(seed), 8)
    solution = scatter_about(key_of[0], (K, 3, NX, NY, NZ), 1.0, 6.0, ((2, 8), (3, 4)), jnp.float32)
    residual = draw_residual(jax.random.fold_in(key_of[7], 71), 0)
    direction = draw_direction(jax.random.fold_in(key_of[7], 71), 0)
    mass = jnp.clip(jnp.exp(math.log(5.0) - 3.218876 * jax.random.uniform(key_of[3], (NX, NY, NZ), jnp.float32) ** levels(key_of[3], (NX, NY, NZ), ((0, 8), (1, 4)), -0.2, 0.2)), 0.2, 5.0)
    coarse_basis = draw_coarse_basis(jax.random.fold_in(key_of[7], 71), 0)
    line_inverse = draw_line_inverse(jax.random.fold_in(key_of[7], 71), 0)
    coarse_factor = draw_coarse_factor(jax.random.fold_in(key_of[7], 71), 0)
    return {"solution": solution, "residual": residual, "direction": direction, "mass": mass, "coarse_basis": coarse_basis, "line_inverse": line_inverse, "coarse_factor": coarse_factor}


exact_mode = lax.Precision.HIGHEST

def shifted(padded, which, offset):
    window = [slice(None), slice(None)]
    for place in (2, 3, 4):
        length = padded.shape[place]
        if place == which:
            window.append(slice(2 + offset, length - 2 + offset))
        else:
            window.append(slice(2, length - 2))
    return padded[tuple(window)]

def apply_operator(padded, mass):
    center = shifted(padded, 2, 0)
    nearby = jnp.zeros_like(center)
    farther = jnp.zeros_like(center)
    for which in (2, 3, 4):
        nearby = nearby + shifted(padded, which, 1) + shifted(padded, which, -1)
        farther = farther + shifted(padded, which, 2) + shifted(padded, which, -2)
    return (mass + 7.5) * center - 4.0 / 3.0 * nearby + 1.0 / 12.0 * farther

def spd_solve(matrix, rhs):
    lower = jnp.linalg.cholesky(matrix)
    middle = lax.linalg.triangular_solve(lower, rhs, left_side=True, lower=True)
    return lax.linalg.triangular_solve(lower, middle, left_side=True, lower=True, transpose_a=True)

def reference(solution, residual, direction, mass, coarse_basis, line_inverse, coarse_factor):
    directions = direction.shape[0]
    shape = direction.shape
    padded = jnp.pad(direction, ((0, 0), (0, 0), (2, 2), (2, 2), (2, 2)))
    image = apply_operator(padded, mass)
    flat_p = direction.reshape(directions, -1)
    flat_q = image.reshape(directions, -1)
    flat_r = residual.reshape(directions, -1)
    gram_pq = jnp.dot(flat_p, flat_q.T, precision=exact_mode)
    proj_pr = jnp.dot(flat_p, flat_r.T, precision=exact_mode)
    alpha_mix = spd_solve(gram_pq, proj_pr)
    new_solution = solution + jnp.dot(alpha_mix.T, flat_p, precision=exact_mode).reshape(shape)
    flat_new = flat_r - jnp.dot(alpha_mix.T, flat_q, precision=exact_mode)
    new_residual = flat_new.reshape(shape)
    blocked = new_residual.reshape(directions, 3, N_SUB, CX, N_INNER, CY, NZ)
    basis_blocked = coarse_basis.reshape(NB, 3, N_SUB, CX, N_INNER, CY, NZ)
    local_part = jnp.einsum('abzw,kcaxbyw->kcaxbyz', line_inverse, blocked, precision=exact_mode)
    coarse_rhs = jnp.einsum('jcaxbyz,kcaxbyz->abjk', basis_blocked, blocked, precision=exact_mode)
    coarse_rhs = coarse_rhs.reshape(NB * N_SUB * N_INNER, directions)
    coarse_mid = jnp.dot(coarse_factor.T, coarse_rhs, precision=exact_mode)
    coarse_sol = jnp.dot(coarse_factor, coarse_mid, precision=exact_mode)
    coarse_sol = coarse_sol.reshape(N_SUB, N_INNER, NB, directions)
    correction = jnp.einsum('jcaxbyz,abjk->kcaxbyz', basis_blocked, coarse_sol, precision=exact_mode)
    precond = (local_part + correction).reshape(directions, -1)
    cross_qz = jnp.dot(flat_q, precond.T, precision=exact_mode)
    beta_mix = -spd_solve(gram_pq, cross_qz)
    new_direction = (precond + jnp.dot(beta_mix.T, flat_p, precision=exact_mode)).reshape(shape)
    return (new_solution, new_residual, new_direction)
```

```python
import functools

import jax
import jax.numpy as jnp
from jax import lax
from jax.experimental import pallas as pl
from jax.experimental.pallas import tpu as pltpu
from jax.sharding import PartitionSpec as P

exact_mode = lax.Precision.HIGHEST
close_mode = lax.Precision.HIGH


def sum_kernel(stages, wide_ref, small_ref, wide_out, small_out, *scratch):
    count = len(stages)
    total, held, small_parts, small_landed = scratch[:4]
    landed = scratch[4 : 4 + count]
    send_sem, recv_sem, small_send, small_recv, back_send, back_recv = scratch[4 + count :]
    bits, partners = ([], [])
    for axis, stride in stages:
        index = lax.axis_index(axis)
        bit = (index // stride) % 2
        bits.append(bit)
        partners.append({axis: index + stride * (1 - 2 * bit)})
    barrier = pltpu.get_barrier_semaphore()
    for partner in partners:
        pl.semaphore_signal(barrier, inc=1, device_id=partner, device_id_type=pl.DeviceIdType.MESH)
    pl.semaphore_wait(barrier, count)

    width = wide_ref.shape[0]
    base = 0
    for t in range(count):
        half = width // 2
        keep = pl.multiple_of(base + bits[t] * half, 8)
        give = pl.multiple_of(base + (1 - bits[t]) * half, 8)
        source = wide_ref if t == 0 else total
        small_source = small_ref if t == 0 else small_parts.at[t - 1]
        small_copy = pltpu.make_async_remote_copy(
            src_ref=small_source,
            dst_ref=small_landed.at[t],
            send_sem=small_send.at[t],
            recv_sem=small_recv.at[t],
            device_id=partners[t],
            device_id_type=pl.DeviceIdType.MESH,
        )
        copy = pltpu.make_async_remote_copy(
            src_ref=source.at[pl.ds(give, half)],
            dst_ref=landed[t],
            send_sem=send_sem.at[t],
            recv_sem=recv_sem.at[t],
            device_id=partners[t],
            device_id_type=pl.DeviceIdType.MESH,
        )
        small_copy.start()
        copy.start()
        small_copy.wait()
        small_sum = small_source[...] + small_landed[t]
        if t < count - 1:
            small_parts[t] = small_sum
        else:
            small_out[...] = small_sum
        copy.wait()
        target = total if t < count - 1 else held
        target[pl.ds(keep, half), :] = source[pl.ds(keep, half), :] + landed[t][...]
        base = base + bits[t] * half
        width = half
    for t in reversed(range(count)):
        mine = pl.ds(pl.multiple_of(base, 8), width)
        copy = pltpu.make_async_remote_copy(
            src_ref=held.at[mine],
            dst_ref=held.at[mine],
            send_sem=back_send.at[t],
            recv_sem=back_recv.at[t],
            device_id=partners[t],
            device_id_type=pl.DeviceIdType.MESH,
        )
        copy.start()
        copy.wait()
        base = base - bits[t] * width
        width = width * 2
    wide_out[...] = held[...]


def sum_everywhere(wide, small, axes):
    stages = []
    for axis in axes:
        stride = 1
        while stride < lax.axis_size(axis):
            stages.append((axis, stride))
            stride *= 2
    count = len(stages)
    rows, lanes = wide.shape
    vmem = pl.BlockSpec(memory_space=pltpu.VMEM)
    dma = pltpu.SemaphoreType.DMA((count,))
    return pl.pallas_call(
        functools.partial(sum_kernel, tuple(stages)),
        out_shape=(
            jax.ShapeDtypeStruct(wide.shape, wide.dtype),
            jax.ShapeDtypeStruct(small.shape, small.dtype),
        ),
        in_specs=[vmem, vmem],
        out_specs=(vmem, vmem),
        scratch_shapes=[
            pltpu.VMEM(wide.shape, wide.dtype),
            pltpu.VMEM(wide.shape, wide.dtype),
            pltpu.VMEM((count,) + small.shape, small.dtype),
            pltpu.VMEM((count,) + small.shape, small.dtype),
            *[pltpu.VMEM((rows >> (t + 1), lanes), wide.dtype) for t in range(count)],
            dma,
            dma,
            dma,
            dma,
            dma,
            dma,
        ],
        compiler_params=pltpu.CompilerParams(collective_id=0, has_side_effects=True),
    )(wide, small)


def with_halo(array, sides, width):
    for axis, dim in sides:
        count, length = (lax.axis_size(axis), array.shape[dim])
        up = [(i, (i + 1) % count) for i in range(count - 1)]
        down = [(j, i) for i, j in up]
        last = lax.slice_in_dim(array, length - width, length, axis=dim)
        initial = lax.slice_in_dim(array, 0, width, axis=dim)
        before = lax.ppermute(last, axis, up)
        after = lax.ppermute(initial, axis, down)
        array = jnp.concatenate([before, array, after], axis=dim)
    return array


def shifted(padded, which, offset):
    window = [slice(None), slice(None)]
    for place in (2, 3, 4):
        length = padded.shape[place]
        if place == which:
            window.append(slice(2 + offset, length - 2 + offset))
        else:
            window.append(slice(2, length - 2))
    return padded[tuple(window)]


def operate(direction, mass):
    widened = with_halo(direction, (("sub", 2), ("inner", 3)), 2)
    padded = jnp.pad(widened, ((0, 0), (0, 0), (0, 0), (0, 0), (2, 2)))
    center = shifted(padded, 2, 0)
    nearby = jnp.zeros_like(center)
    farther = jnp.zeros_like(center)
    for which in (2, 3, 4):
        nearby = nearby + shifted(padded, which, 1) + shifted(padded, which, -1)
        farther = farther + shifted(padded, which, 2) + shifted(padded, which, -2)
    return (mass + 7.5) * center - 4.0 / 3.0 * nearby + 1.0 / 12.0 * farther


def spd_solve(lower, rhs):
    middle = lax.linalg.triangular_solve(lower, rhs, left_side=True, lower=True)
    return lax.linalg.triangular_solve(lower, middle, left_side=True, lower=True, transpose_a=True)


def along_lines(flat, inverse):
    lines = flat.reshape(-1, inverse.shape[0])
    return jnp.dot(lines, inverse.T, precision=close_mode).reshape(flat.shape)


def product(left, right):
    return jnp.dot(left, right.T, precision=exact_mode)


def on_device(solution, residual, direction, mass, coarse_basis, line_inverse, coarse_factor):
    directions = direction.shape[0]
    shape = direction.shape
    inverse = line_inverse[0, 0]
    image = operate(direction, mass)
    flat_p = direction.reshape(directions, -1)
    flat_q = image.reshape(directions, -1)
    flat_r = residual.reshape(directions, -1)
    flat_s = solution.reshape(directions, -1)
    basis_flat = coarse_basis.reshape(coarse_basis.shape[0], -1)
    lined_r = along_lines(flat_r, inverse)
    lined_q = along_lines(flat_q, inverse)
    rhs_r = product(basis_flat, flat_r)
    rhs_q = product(basis_flat, flat_q)
    small = jnp.concatenate(
        [product(flat_p, flat_q), product(flat_p, flat_r), product(flat_q, lined_r), product(flat_q, lined_q)], axis=1
    )
    rhs_both = jnp.concatenate([rhs_r, rhs_q], axis=1)
    half = coarse_factor.shape[1] // 2
    wide = jnp.concatenate(
        [
            jnp.dot(coarse_factor[:, :half].T, rhs_both, precision=exact_mode),
            jnp.dot(coarse_factor[:, half:].T, rhs_both, precision=exact_mode),
        ],
        axis=1,
    )
    wide, small = sum_everywhere(wide, small, ("inner", "sub"))
    gram_pq, proj_pr, image_lined_r, image_lined_q = jnp.split(small, 4, axis=1)
    mids = jnp.concatenate([wide[:, : 2 * directions], wide[:, 2 * directions :]], axis=0)
    mid_r, mid_q = (mids[:, :directions], mids[:, directions:])
    lower = jnp.linalg.cholesky(gram_pq)
    alpha_mix = spd_solve(lower, proj_pr)
    flat_new = flat_r - jnp.dot(alpha_mix.T, flat_q, precision=close_mode)
    local_part = lined_r - jnp.dot(alpha_mix.T, lined_q, precision=close_mode)
    coarse_mid = mid_r - jnp.dot(mid_q, alpha_mix, precision=exact_mode)
    coarse_sol = jnp.dot(coarse_factor, coarse_mid, precision=exact_mode)
    precond = local_part + jnp.dot(coarse_sol.T, basis_flat, precision=close_mode)
    cross_qz = (
        image_lined_r
        - jnp.dot(image_lined_q, alpha_mix, precision=exact_mode)
        + jnp.dot(mid_q.T, coarse_mid, precision=exact_mode)
    )
    new_solution = flat_s + jnp.dot(alpha_mix.T, flat_p, precision=close_mode)
    beta_mix = -spd_solve(lower, cross_qz)
    new_direction = precond + jnp.dot(beta_mix.T, flat_p, precision=close_mode)
    return (new_solution.reshape(shape), flat_new.reshape(shape), new_direction.reshape(shape))


def solution(mesh):
    placed = (
        P(None, None, "sub", "inner", None),
        P(None, None, "sub", "inner", None),
        P(None, None, "sub", "inner", None),
        P("sub", "inner", None),
        P(None, None, "sub", "inner", None),
        P("sub", "inner", None, None),
        P(("sub", "inner"), None),
    )
    return jax.shard_map(
        on_device,
        mesh=mesh,
        in_specs=placed,
        out_specs=(
            P(None, None, "sub", "inner", None),
            P(None, None, "sub", "inner", None),
            P(None, None, "sub", "inner", None),
        ),
        check_vma=False,
    )
```
